128 devices in a mesh: pair: 2 (over core), shard: 64 (over z, y, x).
Axes of the slice: x: 4, y: 4, z: 4, core: 2. Of those that a mesh axis runs over, the one named last changes fastest.
Arguments:
- master: float32 [3072, 4096], P('shard', 'pair'), may hold values from -1.5 to 1.5
- gradient: float32 [3072, 4096], P('shard', 'pair'), may hold values from -40 to 40
- first_moment: float32 [3072, 4096], P('shard', 'pair'), may hold values from -4 to 4
- second_moment: float32 [3072, 4096], P('shard', 'pair'), may hold values from 0.02 to 4
- max_norm: float32 [1], replicated, may hold values from 768 to 1536
- step_count: int32 [1], replicated, may hold values from 1 to 1000
Outputs:
- new_master: float32 [3072, 4096], P('shard', 'pair')
- new_first: float32 [3072, 4096], P('shard', 'pair')
- new_second: float32 [3072, 4096], P('shard', 'pair')
- compute_codes: bfloat16 [3072, 4096], P('pair')
- block_scales: bfloat16 [3072, 128], P('pair')
The draws below stay inside these ranges and needn't reach their ends.
All inputs are finite; a program needn't handle non-finite values.
Results may differ from the reference program's by a relative error of at most 0.001.
The reference program's roundings to bfloat16 on the way count: a program that leaves them out, or rounds other values in their place, can miss the bound.
Values may be sent and summed in bfloat16 or wider, within the bound.
A program may use at most 192 MiB of HBM per device.

```python
import math
import jax
import jax.numpy as jnp
from jax import lax

ROWS = 3072
COLS = 4096
BLOCK = 32


def draw_gradient(key, part):
    key_heads, key_halves, key_rows, key_noise = jax.random.split(key, 4)
    head_count = (ROWS + 127) // 128
    head_index = jnp.arange(ROWS) // 128
    head_log = jax.random.uniform(key_heads, (head_count,), minval=-2.0, maxval=2.0)
    head_scale = jnp.exp(head_log)[head_index][:, None]
    half_sign = jnp.where(jax.random.bernoulli(key_halves), 1.0, -1.0)
    upper_half = jnp.arange(COLS) >= COLS // 2
    half_scale = jnp.exp(0.7 * half_sign * jnp.where(upper_half, -1.0, 1.0))[None, :]
    row_scale = jnp.exp(jax.random.uniform(key_rows, (ROWS, 1), minval=-0.7, maxval=0.7))
    noise_part = jnp.clip(jax.random.normal(key_noise, (ROWS, COLS)), -6.0, 6.0)
    values = head_scale * half_scale * row_scale * noise_part
    return jnp.clip(values, -40.0, 40.0).astype(jnp.float32)


def block_scale(key, dims, cuts, low, high):
    def one(axis_at, parts):
        heights = jax.random.uniform(jax.random.fold_in(jax.random.fold_in(key, 6), axis_at), (parts,), jnp.float32, low / len(cuts), high / len(cuts))
        return jnp.repeat(jnp.exp(heights), dims[axis_at] // parts).reshape((-1,) + (1,) * (len(dims) - axis_at - 1))

    gain = one(*cuts[0])
    for cut in cuts[1:]:
        gain = gain * one(*cut)
    return gain


def noise(rng, extent, scale, limit, pieces=(), kind=jnp.bfloat16):
    loudness = block_scale(rng, extent, pieces, -0.22, 0.18) if pieces else 1.0
    drawn = jax.random.normal(rng, extent, jnp.float32) * scale * loudness
    return jnp.minimum(jnp.maximum(drawn, -limit), limit).astype(kind)


def setup_inputs(seed: int = 0) -> dict:
    streams_of = jax.random.split(jax.random.key(seed), 7)
    return {
        "master": noise(streams_of[0], (ROWS, COLS), 0.25, 1.5, ((0, 64), (1, 2)), jnp.float32),
        "gradient": draw_gradient(jax.random.fold_in(streams_of[6], 71), 0),
        "first_moment": noise(streams_of[2], (ROWS, COLS), 0.5, 4.0, ((0, 64), (1, 2)), jnp.float32),
        "second_moment": jnp.clip(jnp.exp(math.log(4.0) - 5.2983174 * jax.random.uniform(streams_of[3], (ROWS, COLS), jnp.float32) ** block_scale(streams_of[3], (ROWS, COLS), ((0, 64), (1, 2)), -0.2, 0.2)), 0.02, 4.0),
        "max_norm": jnp.clip(jax.random.uniform(streams_of[4], (1,), jnp.float32, 768.0, 1536.0), 768.0, 1536.0),
        "step_count": jax.random.randint(streams_of[5], (1,), 1, 1001).astype(jnp.int32),
    }


beta_first = 0.9
beta_second = 0.99
learn_rate = 0.01
decay_rate = 0.1
adam_eps = 1e-06
scale_floor = 0.25

def quantize(weights):
    height, width = weights.shape
    blocked = weights.reshape(height, width // BLOCK, BLOCK)
    largest = lax.optimization_barrier(jnp.max(jnp.abs(blocked), axis=2))
    scales = jnp.maximum(largest, scale_floor).astype(jnp.bfloat16)
    divided = blocked / scales.astype(jnp.float32)[:, :, None]
    return (divided.astype(jnp.bfloat16).reshape(height, width), scales)

def adam_update(master, gradient, first_moment, second_moment, max_norm, step_count, squares):
    norm_limit = max_norm[0]
    clip_factor = norm_limit / jnp.maximum(jnp.sqrt(squares), norm_limit)
    clipped = clip_factor * gradient
    new_first = beta_first * first_moment + (1.0 - beta_first) * clipped
    new_second = beta_second * second_moment + (1.0 - beta_second) * clipped * clipped
    counted = step_count[0].astype(jnp.float32)
    first_fix = 1.0 - jnp.power(jnp.full((), beta_first, jnp.float32), counted)
    second_fix = 1.0 - jnp.power(jnp.full((), beta_second, jnp.float32), counted)
    update = new_first / first_fix / (jnp.sqrt(new_second / second_fix) + adam_eps) + decay_rate * master
    new_master = master - learn_rate * update
    return (new_master, new_first, new_second)

def reference(master, gradient, first_moment, second_moment, max_norm, step_count):
    squares = jnp.sum(gradient * gradient)
    new_master, new_first, new_second = adam_update(master, gradient, first_moment, second_moment, max_norm, step_count, squares)
    compute_codes, block_scales = quantize(new_master)
    return (new_master, new_first, new_second, compute_codes, block_scales)
```

```python
import functools
import heapq
import itertools

import jax
import jax.numpy as jnp
import numpy as np
from jax import lax
from jax.experimental import pallas as pl
from jax.experimental.pallas import tpu as pltpu
from jax.sharding import PartitionSpec as P

MESH = pl.DeviceIdType.MESH
F32, BF16 = jnp.float32, jnp.bfloat16

beta_first = 0.9
beta_second = 0.99
learn_rate = 0.01
decay_rate = 0.1
adam_eps = 1e-06
scale_floor = 0.25

BLOCK = 32
PART = 16
LANES = 128
ORDERS = ((0, 1, 2), (1, 2, 0), (2, 0, 1))


def hops(part, plane, off):
    order = ORDERS[part]
    last = max([j for j, d in enumerate(order) if off[d]], default=-1)
    out = []
    if last >= 0:
        d = order[last]
        swap = d == 2 and plane == 1
        if off[d] == 1:
            out.append((d, 1, 2 if swap else 1))
        if off[d] == 3:
            out.append((d, -1, 1 if swap else 2))
    for d in order[last + 1 :]:
        out += [(d, 1, 0), (d, -1, 0)]
    return out


def arrivals(unit=1.45, latency=1.7, ready=(0.6, 1.2, 1.8)):
    queues = {(r, d, s): [] for r in range(4) for d in range(3) for s in (1, -1)}
    heads, events, count, now = {}, [], itertools.count(), 0.0
    got = {r: {} for r in range(4)}
    order = {r: [] for r in range(4)}
    for r in (0, 1):
        for p in range(3):
            heapq.heappush(events, (ready[p], next(count), r, (p, r, 0, 0), 0))
    while True:
        for k in queues:
            if k not in heads and queues[k]:
                item = queues[k].pop(0)
                heads[k] = [unit if item[1] == 0 else unit / 2, item]
        rate = {k: 0.5 if ((k[0] + 2) % 4, k[1], k[2]) in heads else 1.0 for k in heads}
        times = [now + heads[k][0] / rate[k] for k in heads] + ([events[0][0]] if events else [])
        if not times:
            return order
        then = min(times)
        for k in heads:
            heads[k][0] -= (then - now) * rate[k]
        now = then
        for k in list(heads):
            if heads[k][0] <= 1e-9:
                (r, d, s), ((p, plane, ox, oy), half) = k, heads.pop(k)[1]
                if d == 0:
                    ox = (ox + s) % 4
                elif d == 1:
                    oy = (oy + s) % 4
                else:
                    r = (r + s) % 4
                heapq.heappush(events, (now + latency, next(count), r, (p, plane, ox, oy), half))
        while events and events[0][0] <= now + 1e-9:
            _, _, r, chunk, half = heapq.heappop(events)
            p, plane, ox, oy = chunk
            off = (ox, oy, (r - plane) % 4)
            if off != (0, 0, 0):
                order[r].append((chunk, half))
            seen = got[r].setdefault(chunk, set())
            seen.add(half)
            if 0 in seen or len(seen) == 2:
                for d, s, h in hops(p, plane, off):
                    queues[(r, d, s)].append((chunk, h))


def slot(chunk, half):
    p, plane, ox, oy = chunk
    return (((p * 2 + plane) * 4 + ox) * 4 + oy) * 2 + (half == 2)


SLOTS = 3 * 2 * 4 * 4 * 2


def gather_kernel(
    max_norm,
    step_count,
    master,
    gradient,
    first,
    second,
    new_master,
    new_first,
    new_second,
    whole,
    own,
    other,
    sums,
    sum_rx,
    load_sem,
    swap_sem,
    sum_send,
    sum_recv,
    send_sem,
    recv_sem,
):
    rows, width = own.shape[1:]
    parts = rows // PART
    cols = 2 * width
    full = whole.shape[1]
    cut = LANES * ((full // LANES + 1) // 2)

    me = lax.axis_index("shard")
    core = lax.axis_index("pair")
    x, y, z = lax.rem(me, 4), lax.rem(lax.div(me, 4), 4), lax.div(me, 16)
    role = lax.rem(z + 2 * core, 4)
    source = role < 2
    flip = jnp.logical_or(role == 1, role == 2)
    sigma = jnp.where(flip, -1, 1)

    def at(xx, yy, zz):
        return lax.rem(zz, 4) * 16 + lax.rem(yy, 4) * 4 + lax.rem(xx, 4)

    partner = (1 - core, me)
    x_peers = [(k, at(x + dx, y, z)) for dx in (1, 2, 3) for k in (core, 1 - core)] + [partner]
    y_peers = [(core, at(x, y + d, z)) for d in (1, 2, 3)]
    z_peers = [(core, at(x, y, z + d)) for d in (1, 2, 3)]
    barrier = pltpu.get_barrier_semaphore()
    peers = x_peers + y_peers + z_peers
    for peer in peers:
        pl.semaphore_signal(barrier, inc=1, device_id=peer, device_id_type=MESH)

    loads = [
        pltpu.make_async_copy(ref, own.at[k], load_sem.at[k])
        for k, ref in enumerate((gradient, first, second, master))
    ]
    for load in loads:
        load.start()
    loads[0].wait()
    acc = jnp.zeros((8, LANES), F32)
    for i in range(0, rows, 8):
        for j in range(0, width, LANES):
            g = own[0, i : i + 8, j : j + LANES]
            acc = acc + g * g
    sums[0] = acc
    for load in loads[1:]:
        load.wait()
    pl.semaphore_wait(barrier, len(peers))

    def exchange(step, base, to):
        copies = [
            pltpu.make_async_remote_copy(
                src_ref=sums.at[step],
                dst_ref=sum_rx.at[base + k],
                send_sem=sum_send.at[base + k],
                recv_sem=sum_recv.at[base + k],
                device_id=peer,
                device_id_type=MESH,
            )
            for k, peer in enumerate(to)
        ]
        for copy in copies:
            copy.start()
        return copies

    swaps = [
        pltpu.make_async_remote_copy(
            src_ref=own.at[k],
            dst_ref=other.at[k],
            send_sem=swap_sem.at[k],
            recv_sem=swap_sem.at[4 + k],
            device_id=partner,
            device_id_type=MESH,
        )
        for k in range(4)
    ]

    copies = []
    base = 0
    for step, to in enumerate((x_peers, y_peers, z_peers)):
        started = exchange(step, base, to)
        if step == 0:

            @pl.when(jnp.logical_not(source))
            def _():
                for swap in swaps:
                    swap.start()

        for k, copy in enumerate(started):
            copy.wait_recv()
        acc = sums[step]
        for k in range(len(to)):
            acc = acc + sum_rx[base + k]
        base += len(to)
        copies += started
        if step < 2:
            sums[step + 1] = acc

    squares = jnp.sum(acc, axis=(0, 1), keepdims=True)
    limit = jnp.full((1, 1), max_norm[0], F32)
    clip = limit / jnp.maximum(jnp.sqrt(squares), limit)
    counted = jnp.full((1, 1), step_count[0], jnp.int32).astype(F32)
    inv_first = 1.0 / (1.0 - jnp.exp(counted * float(np.log(beta_first))))
    inv_second = 1.0 / (1.0 - jnp.exp(counted * float(np.log(beta_second))))
    clip = jnp.broadcast_to(clip, (PART, LANES))
    inv_first = jnp.broadcast_to(inv_first, (PART, LANES))
    inv_second = jnp.broadcast_to(inv_second, (PART, LANES))

    lane = lax.broadcasted_iota(jnp.int32, (PART, LANES), 1)
    bits = [(s, lax.bitwise_and(lane, s) != 0) for s in (1, 2, 4, 8, 16)]
    in_block = lax.bitwise_and(lane, BLOCK - 1)
    to_lane = lax.broadcasted_iota(jnp.int32, (LANES, LANES), 1)
    from_lane = lax.broadcasted_iota(jnp.int32, (LANES, LANES), 0)
    spread = jnp.where(
        lax.div(from_lane, BLOCK) + (LANES // BLOCK) * lax.rem(from_lane, BLOCK) == to_lane, 1.0, 0.0
    ).astype(BF16)

    def adam(held, i, j):
        g, m, v, w = (held[k, pl.ds(i, PART), pl.ds(j, LANES)] for k in range(4))
        clipped = clip * g
        m = beta_first * m + (1.0 - beta_first) * clipped
        v = beta_second * v + (1.0 - beta_second) * clipped * clipped
        update = m * inv_first / (jnp.sqrt(v * inv_second) + adam_eps) + decay_rate * w
        return w - learn_rate * update, m, v

    tiles = width // LANES
    step_tiles = 4

    def store(i, j, w, m, v):
        new_master[pl.ds(i, PART), pl.ds(j, LANES)] = w
        new_first[pl.ds(i, PART), pl.ds(j, LANES)] = m
        new_second[pl.ds(i, PART), pl.ds(j, LANES)] = v

    def quantize(row, half, tile, w, scales):
        largest = jnp.abs(w)
        for s, bit in bits:
            lower = pltpu.roll(largest, s, 1)
            upper = pltpu.roll(largest, LANES - s, 1)
            largest = jnp.maximum(largest, jnp.where(bit, lower, upper))
        scale = jnp.maximum(largest, scale_floor).astype(BF16).astype(F32)
        column = pl.multiple_of(half * width + tile * LANES, LANES)
        whole[pl.ds(row, PART), pl.ds(column, LANES)] = (w / scale).astype(BF16)
        return jnp.where(in_block == half * tiles + tile, scale, scales)

    line = [[(lax.rem(y + 4 - oy, 4) * 4 + lax.rem(x + 4 - ox, 4)) * rows for oy in range(4)] for ox in range(4)]
    plane_row = [jnp.where(flip, 16 * rows, 0), jnp.where(flip, 0, 16 * rows)]
    near = {
        (0, 1): at(x + 1, y, z),
        (0, -1): at(x + 3, y, z),
        (1, 1): at(x, y + 1, z),
        (1, -1): at(x, y + 3, z),
        (2, 1): at(x, y, z + 4 + sigma),
        (2, -1): at(x, y, z + 4 - sigma),
    }
    pieces = {0: pl.ds(0, full), 1: pl.ds(0, cut), 2: pl.ds(cut, full - cut)}

    def place(chunk, half):
        p, plane, ox, oy = chunk
        return whole.at[pl.ds(pl.multiple_of(line[ox][oy] + plane_row[plane] + p * PART, PART), PART), pieces[half]]

    def piece(chunk, half, role_now, d, s, number):
        p, plane, ox, oy = chunk
        if d == 0:
            ox = (ox + s) % 4
        elif d == 1:
            oy = (oy + s) % 4
        elif (role_now == 0) == (s == 1):
            plane = 1 - plane
        ref = place(chunk, half)
        return pltpu.make_async_remote_copy(
            src_ref=ref,
            dst_ref=ref,
            send_sem=send_sem.at[number],
            recv_sem=recv_sem.at[slot((p, plane, ox, oy), half)],
            device_id=(core, near[(d, s)]),
            device_id_type=MESH,
        )

    def landed(chunk, half):
        ref = place(chunk, half)
        pltpu.make_async_remote_copy(
            src_ref=ref,
            dst_ref=ref,
            send_sem=send_sem.at[0],
            recv_sem=recv_sem.at[slot(chunk, half)],
            device_id=(core, near[(0, 1)]),
            device_id_type=MESH,
        ).wait_recv()

    def follow(role_now, order, sent):
        got = {}
        for chunk, half in order:
            landed(chunk, half)
            seen = got.setdefault(chunk, set())
            seen.add(half)
            if 0 in seen or len(seen) == 2:
                p, plane, ox, oy = chunk
                for d, s, h in hops(p, plane, (ox, oy, (role_now - plane) % 4)):
                    copy = piece(chunk, h, role_now, d, s, len(sent))
                    copy.start()
                    sent.append(copy)
        for copy in sent:
            copy.wait_send()

    schedule = arrivals()

    @pl.when(source)
    def _():
        for swap in swaps:
            swap.wait_recv()
        sent = []
        for p in range(parts):
            i = p * PART
            row = pl.multiple_of(line[0][0] + plane_row[0] + i, PART)

            def body(t, scales, i=i, row=row):
                for k in range(step_tiles):
                    tile = t * step_tiles + k
                    j = pl.multiple_of(tile * LANES, LANES)
                    w, m, v = adam(own, i, j)
                    store(i, j, w, m, v)
                    scales = quantize(row, core, tile, w, scales)
                    w, m, v = adam(other, i, j)
                    scales = quantize(row, 1 - core, tile, w, scales)
                return scales

            scales = lax.fori_loop(0, tiles // step_tiles, body, jnp.zeros((PART, LANES), F32))
            moved = jnp.dot(scales.astype(BF16), spread, preferred_element_type=F32)
            whole[pl.ds(row, PART), cols:] = moved.astype(BF16)
            for d, s, h in hops(p, 0, (0, 0, 0)):
                copy = piece((p, 0, 0, 0), h, 0, d, s, len(sent))
                copy.start()
                sent.append(copy)
        follow(0, schedule[0], sent)

    @pl.when(jnp.logical_not(source))
    def _():
        for p in range(parts):
            i = p * PART

            def body(t, carry, i=i):
                for k in range(step_tiles):
                    j = pl.multiple_of((t * step_tiles + k) * LANES, LANES)
                    store(i, j, *adam(own, i, j))
                return carry

            lax.fori_loop(0, tiles // step_tiles, body, 0)
        follow(3, schedule[3], [])
        for swap in swaps:
            swap.wait_send()

    for copy in copies:
        copy.wait_send()


def write_kernel(whole, new_master, new_first, new_second, codes_out, scales_out, master_out, first_out, second_out, sem):
    rows, cols = codes_out.shape
    count = 8
    step = rows // count
    copies = []

    def go(src, dst):
        copy = pltpu.make_async_copy(src, dst, sem.at[len(copies)])
        copy.start()
        copies.append(copy)

    for k in range(count):
        go(whole.at[pl.ds(k * step, step), pl.ds(0, cols)], codes_out.at[pl.ds(k * step, step), :])
    go(whole.at[:, pl.ds(cols, scales_out.shape[1])], scales_out)
    go(new_master, master_out)
    go(new_first, first_out)
    go(new_second, second_out)
    for copy in copies:
        copy.wait()


def per_device(master, gradient, first_moment, second_moment, max_norm, step_count):
    rows, width = master.shape
    cols = 2 * width
    scales = cols // BLOCK
    kept = 32 * rows
    full = cols + scales
    smem = pl.BlockSpec(memory_space=pltpu.SMEM)
    any_spec = pl.BlockSpec(memory_space=pl.ANY)
    vmem = pl.BlockSpec(memory_space=pltpu.VMEM)
    sends = 160
    held = pl.pallas_call(
        gather_kernel,
        out_shape=tuple(pltpu.VMEM((rows, width), F32) for _ in range(3)) + (pltpu.VMEM((kept, full), BF16),),
        in_specs=[smem, smem] + [any_spec] * 4,
        out_specs=tuple(vmem for _ in range(4)),
        scratch_shapes=[
            pltpu.VMEM((4, rows, width), F32),
            pltpu.VMEM((4, rows, width), F32),
            pltpu.VMEM((3, 8, LANES), F32),
            pltpu.VMEM((13, 8, LANES), F32),
            pltpu.SemaphoreType.DMA((4,)),
            pltpu.SemaphoreType.DMA((8,)),
            pltpu.SemaphoreType.DMA((13,)),
            pltpu.SemaphoreType.DMA((13,)),
            pltpu.SemaphoreType.DMA((sends,)),
            pltpu.SemaphoreType.DMA((SLOTS,)),
        ],
        compiler_params=pltpu.CompilerParams(collective_id=0, has_side_effects=True, vmem_limit_bytes=16 * 2**20),
        name="update_and_gather",
    )(
        max_norm,
        step_count,
        *(
            pltpu.with_memory_space_constraint(a, pltpu.HBM)
            for a in (master, gradient, first_moment, second_moment)
        ),
    )
    new_master, new_first, new_second, whole = (
        pltpu.with_memory_space_constraint(a, pltpu.VMEM) for a in held
    )
    codes, block_scales, new_master, new_first, new_second = pl.pallas_call(
        write_kernel,
        out_shape=(
            jax.ShapeDtypeStruct((kept, cols), BF16),
            jax.ShapeDtypeStruct((kept, scales), BF16),
        )
        + tuple(jax.ShapeDtypeStruct((rows, width), F32) for _ in range(3)),
        in_specs=[vmem] * 4,
        out_specs=tuple(any_spec for _ in range(5)),
        scratch_shapes=[pltpu.SemaphoreType.DMA((12,))],
        compiler_params=pltpu.CompilerParams(vmem_limit_bytes=16 * 2**20),
        name="write_results",
    )(whole, new_master, new_first, new_second)
    return (new_master, new_first, new_second, codes, block_scales)


def solution(mesh):
    return jax.shard_map(
        per_device,
        mesh=mesh,
        in_specs=(P("shard", "pair"),) * 4 + (P(), P()),
        out_specs=(P("shard", "pair"),) * 3 + (P("pair", None),) * 2,
        check_vma=False,
    )
```

```python
import functools
import heapq
import itertools

import jax
import jax.numpy as jnp
import numpy as np
from jax import lax
from jax.experimental import pallas as pl
from jax.experimental.pallas import tpu as pltpu
from jax.sharding import PartitionSpec as P

MESH = pl.DeviceIdType.MESH
F32, BF16 = jnp.float32, jnp.bfloat16

beta_first = 0.9
beta_second = 0.99
learn_rate = 0.01
decay_rate = 0.1
adam_eps = 1e-06
scale_floor = 0.25

BLOCK = 32
PART = 16
LANES = 128
ORDERS = ((0, 1, 2), (1, 2, 0), (2, 0, 1))


def hops(part, plane, off):
    order = ORDERS[part]
    last = max([j for j, d in enumerate(order) if off[d]], default=-1)
    out = []
    if last >= 0:
        d = order[last]
        swap = d == 2 and plane == 1
        if off[d] == 1:
            out.append((d, 1, 2 if swap else 1))
        if off[d] == 3:
            out.append((d, -1, 1 if swap else 2))
    for d in order[last + 1 :]:
        out += [(d, 1, 0), (d, -1, 0)]
    return out


def arrivals(unit=1.45, latency=1.7, ready=(0.6, 1.2, 1.8)):
    queues = {(r, d, s): [] for r in range(4) for d in range(3) for s in (1, -1)}
    heads, events, count, now = {}, [], itertools.count(), 0.0
    got = {r: {} for r in range(4)}
    order = {r: [] for r in range(4)}
    for r in (0, 1):
        for p in range(3):
            heapq.heappush(events, (ready[p], next(count), r, (p, r, 0, 0), 0))
    while True:
        for k in queues:
            if k not in heads and queues[k]:
                item = queues[k].pop(0)
                heads[k] = [unit if item[1] == 0 else unit / 2, item]
        rate = {k: 0.5 if ((k[0] + 2) % 4, k[1], k[2]) in heads else 1.0 for k in heads}
        times = [now + heads[k][0] / rate[k] for k in heads] + ([events[0][0]] if events else [])
        if not times:
            return order
        then = min(times)
        for k in heads:
            heads[k][0] -= (then - now) * rate[k]
        now = then
        for k in list(heads):
            if heads[k][0] <= 1e-9:
                (r, d, s), ((p, plane, ox, oy), half) = k, heads.pop(k)[1]
                if d == 0:
                    ox = (ox + s) % 4
                elif d == 1:
                    oy = (oy + s) % 4
                else:
                    r = (r + s) % 4
                heapq.heappush(events, (now + latency, next(count), r, (p, plane, ox, oy), half))
        while events and events[0][0] <= now + 1e-9:
            _, _, r, chunk, half = heapq.heappop(events)
            p, plane, ox, oy = chunk
            off = (ox, oy, (r - plane) % 4)
            if off != (0, 0, 0):
                order[r].append((chunk, half))
            seen = got[r].setdefault(chunk, set())
            seen.add(half)
            if 0 in seen or len(seen) == 2:
                for d, s, h in hops(p, plane, off):
                    queues[(r, d, s)].append((chunk, h))


def slot(chunk, half):
    p, plane, ox, oy = chunk
    return (((p * 2 + plane) * 4 + ox) * 4 + oy) * 2 + (half == 2)


SLOTS = 3 * 2 * 4 * 4 * 2


def gather_kernel(
    max_norm,
    step_count,
    master,
    gradient,
    first,
    second,
    new_master,
    new_first,
    new_second,
    whole,
    own,
    other,
    fresh,
    largest,
    sums,
    sum_rx,
    load_sem,
    swap_sem,
    sum_send,
    sum_recv,
    send_sem,
    recv_sem,
):
    rows, width = own.shape[1:]
    parts = rows // PART
    cols = 2 * width
    full = whole.shape[1]
    cut = LANES * ((full // LANES + 1) // 2)

    me = lax.axis_index("shard")
    core = lax.axis_index("pair")
    x, y, z = lax.rem(me, 4), lax.rem(lax.div(me, 4), 4), lax.div(me, 16)
    role = lax.rem(z + 2 * core, 4)
    source = role < 2
    flip = jnp.logical_or(role == 1, role == 2)
    sigma = jnp.where(flip, -1, 1)

    def at(xx, yy, zz):
        return lax.rem(zz, 4) * 16 + lax.rem(yy, 4) * 4 + lax.rem(xx, 4)

    partner = (1 - core, me)
    x_peers = [(k, at(x + dx, y, z)) for dx in (1, 2, 3) for k in (core, 1 - core)] + [partner]
    y_peers = [(core, at(x, y + d, z)) for d in (1, 2, 3)]
    z_peers = [(core, at(x, y, z + d)) for d in (1, 2, 3)]
    barrier = pltpu.get_barrier_semaphore()
    peers = x_peers + y_peers + z_peers
    for peer in peers:
        pl.semaphore_signal(barrier, inc=1, device_id=peer, device_id_type=MESH)

    loads = [
        pltpu.make_async_copy(ref, own.at[k], load_sem.at[k])
        for k, ref in enumerate((gradient, first, second, master))
    ]
    for load in loads:
        load.start()
    loads[0].wait()
    acc = jnp.zeros((8, LANES), F32)
    for i in range(0, rows, 8):
        for j in range(0, width, LANES):
            g = own[0, i : i + 8, j : j + LANES]
            acc = acc + g * g
    sums[0] = acc
    for load in loads[1:]:
        load.wait()
    pl.semaphore_wait(barrier, len(peers))

    def exchange(step, base, to):
        copies = [
            pltpu.make_async_remote_copy(
                src_ref=sums.at[step],
                dst_ref=sum_rx.at[base + k],
                send_sem=sum_send.at[step],
                recv_sem=sum_recv.at[step],
                device_id=peer,
                device_id_type=MESH,
            )
            for k, peer in enumerate(to)
        ]
        for copy in copies:
            copy.start()
        slots = sum_rx.at[pl.ds(base, len(to))]
        return pltpu.make_async_remote_copy(
            src_ref=slots,
            dst_ref=slots,
            send_sem=sum_send.at[step],
            recv_sem=sum_recv.at[step],
            device_id=to[0],
            device_id_type=MESH,
        )

    swap = pltpu.make_async_remote_copy(
        src_ref=own,
        dst_ref=other,
        send_sem=swap_sem.at[0],
        recv_sem=swap_sem.at[1],
        device_id=partner,
        device_id_type=MESH,
    )

    exchanges = []
    base = 0
    for step, to in enumerate((x_peers, y_peers, z_peers)):
        started = exchange(step, base, to)
        if step == 0:

            @pl.when(jnp.logical_not(source))
            def _():
                swap.start()

        started.wait_recv()
        acc = sums[step]
        for k in range(len(to)):
            acc = acc + sum_rx[base + k]
        base += len(to)
        exchanges.append(started)
        if step < 2:
            sums[step + 1] = acc

    squares = jnp.sum(acc, axis=(0, 1), keepdims=True)
    limit = jnp.full((1, 1), max_norm[0], F32)
    clip = limit / jnp.maximum(jnp.sqrt(squares), limit)
    counted = jnp.full((1, 1), step_count[0], jnp.int32).astype(F32)
    inv_first = 1.0 / (1.0 - jnp.exp(counted * float(np.log(beta_first))))
    inv_second = 1.0 / (1.0 - jnp.exp(counted * float(np.log(beta_second))))
    clip = jnp.broadcast_to(clip, (PART, LANES))
    inv_first = jnp.broadcast_to(inv_first, (PART, LANES))
    inv_second = jnp.broadcast_to(inv_second, (PART, LANES))

    lane = lax.broadcasted_iota(jnp.int32, (PART, LANES), 1)
    block_start = lane - lax.bitwise_and(lane, BLOCK - 1)
    to_lane = lax.broadcasted_iota(jnp.int32, (LANES, LANES), 1)
    from_lane = lax.broadcasted_iota(jnp.int32, (LANES, LANES), 0)
    spread = jnp.where(
        lax.div(from_lane, BLOCK) + (LANES // BLOCK) * lax.rem(from_lane, BLOCK) == to_lane, 1.0, 0.0
    ).astype(BF16)

    def adam(held, i, j):
        g, m, v, w = (held[k, pl.ds(i, PART), pl.ds(j, LANES)] for k in range(4))
        clipped = clip * g
        m = beta_first * m + (1.0 - beta_first) * clipped
        v = beta_second * v + (1.0 - beta_second) * clipped * clipped
        update = m * inv_first / (jnp.sqrt(v * inv_second) + adam_eps) + decay_rate * w
        return w - learn_rate * update, m, v

    tiles = width // LANES
    step_tiles = 4

    def store(i, j, w, m, v):
        new_master[pl.ds(i, PART), pl.ds(j, LANES)] = w
        new_first[pl.ds(i, PART), pl.ds(j, LANES)] = m
        new_second[pl.ds(i, PART), pl.ds(j, LANES)] = v

    def merge(a, b, bit):
        here = lax.bitwise_and(lane, bit) != 0
        crossed = jnp.where(here, a, b)
        crossed = jnp.where(here, pltpu.roll(crossed, bit, 1), pltpu.roll(crossed, LANES - bit, 1))
        return jnp.maximum(jnp.where(here, b, a), crossed)

    def merge_all(values, bit):
        while len(values) > 1:
            values = [merge(a, b, bit) for a, b in zip(values[::2], values[1::2])]
            bit *= 2
        return values[0]

    def update_chunk(i, row):
        def update(t, carry):
            for half, held in enumerate((own, other)):
                at_half = core if half == 0 else 1 - core
                sizes = []
                for k in range(step_tiles):
                    j = pl.multiple_of((t * step_tiles + k) * LANES, LANES)
                    w, m, v = adam(held, i, j)
                    if half == 0:
                        store(i, j, w, m, v)
                    fresh[:, pl.ds(pl.multiple_of(at_half * width + j, LANES), LANES)] = w
                    sizes.append(jnp.abs(w))
                largest[half, t] = merge_all(sizes, 1)
            return carry

        lax.fori_loop(0, tiles // step_tiles, update, 0)
        mine, others = (merge_all([largest[h, t] for t in range(tiles // step_tiles)], step_tiles) for h in (0, 1))
        top = merge(jnp.where(core == 0, mine, others), jnp.where(core == 0, others, mine), tiles)
        scales = jnp.maximum(top, scale_floor).astype(BF16)
        whole[pl.ds(row, PART), cols:] = jnp.dot(scales, spread, preferred_element_type=F32).astype(BF16)
        inverse = 1.0 / scales.astype(F32)

        def code(t, carry):
            for k in range(2 * step_tiles):
                tile = t * 2 * step_tiles + k
                j = pl.ds(pl.multiple_of(tile * LANES, LANES), LANES)
                by = jnp.take_along_axis(inverse, block_start + tile, axis=1, mode="promise_in_bounds")
                whole[pl.ds(row, PART), j] = (fresh[:, j] * by).astype(BF16)
            return carry

        lax.fori_loop(0, tiles // step_tiles, code, 0)

    line = [[(lax.rem(y + 4 - oy, 4) * 4 + lax.rem(x + 4 - ox, 4)) * rows for oy in range(4)] for ox in range(4)]
    plane_row = [jnp.where(flip, 16 * rows, 0), jnp.where(flip, 0, 16 * rows)]
    near = {
        (0, 1): at(x + 1, y, z),
        (0, -1): at(x + 3, y, z),
        (1, 1): at(x, y + 1, z),
        (1, -1): at(x, y + 3, z),
        (2, 1): at(x, y, z + 4 + sigma),
        (2, -1): at(x, y, z + 4 - sigma),
    }
    pieces = {0: pl.ds(0, full), 1: pl.ds(0, cut), 2: pl.ds(cut, full - cut)}

    def place(chunk, half):
        p, plane, ox, oy = chunk
        return whole.at[pl.ds(pl.multiple_of(line[ox][oy] + plane_row[plane] + p * PART, PART), PART), pieces[half]]

    def lane_of(d, s, half):
        return (d * 2 + (s < 0)) * 3 + half

    def piece(chunk, half, role_now, d, s):
        p, plane, ox, oy = chunk
        if d == 0:
            ox = (ox + s) % 4
        elif d == 1:
            oy = (oy + s) % 4
        elif (role_now == 0) == (s == 1):
            plane = 1 - plane
        ref = place(chunk, half)
        return pltpu.make_async_remote_copy(
            src_ref=ref,
            dst_ref=ref,
            send_sem=send_sem.at[lane_of(d, s, half)],
            recv_sem=recv_sem.at[slot((p, plane, ox, oy), half)],
            device_id=(core, near[(d, s)]),
            device_id_type=MESH,
        )

    def landed(chunk, half):
        ref = place(chunk, half)
        pltpu.make_async_remote_copy(
            src_ref=ref,
            dst_ref=ref,
            send_sem=send_sem.at[0],
            recv_sem=recv_sem.at[slot(chunk, half)],
            device_id=(core, near[(0, 1)]),
            device_id_type=MESH,
        ).wait_recv()

    def follow(role_now, order, sent):
        got = {}
        for chunk, half in order:
            landed(chunk, half)
            seen = got.setdefault(chunk, set())
            seen.add(half)
            if 0 in seen or len(seen) == 2:
                p, plane, ox, oy = chunk
                for d, s, h in hops(p, plane, (ox, oy, (role_now - plane) % 4)):
                    piece(chunk, h, role_now, d, s).start()
                    sent.append((d, s, h))
        for d, s, h in sorted(set(sent)):
            total = whole.at[pl.ds(0, PART * sent.count((d, s, h))), pieces[h]]
            pltpu.make_async_remote_copy(
                src_ref=total,
                dst_ref=total,
                send_sem=send_sem.at[lane_of(d, s, h)],
                recv_sem=recv_sem.at[0],
                device_id=(core, near[(d, s)]),
                device_id_type=MESH,
            ).wait_send()

    schedule = arrivals()

    @pl.when(source)
    def _():
        swap.wait_recv()
        sent = []
        for p in range(parts):
            i = p * PART
            row = pl.multiple_of(line[0][0] + plane_row[0] + i, PART)

            update_chunk(i, row)
            for d, s, h in hops(p, 0, (0, 0, 0)):
                piece((p, 0, 0, 0), h, 0, d, s).start()
                sent.append((d, s, h))
        follow(0, schedule[0], sent)

    @pl.when(jnp.logical_not(source))
    def _():
        for p in range(parts):
            i = p * PART

            def body(t, carry, i=i):
                for k in range(step_tiles):
                    j = pl.multiple_of((t * step_tiles + k) * LANES, LANES)
                    store(i, j, *adam(own, i, j))
                return carry

            lax.fori_loop(0, tiles // step_tiles, body, 0)
        follow(3, schedule[3], [])
        swap.wait_send()

    for started in exchanges:
        started.wait_send()


def write_kernel(whole, new_master, new_first, new_second, codes_out, scales_out, master_out, first_out, second_out, sem):
    rows, cols = codes_out.shape
    count = 8
    step = rows // count
    copies = []

    def go(src, dst):
        copy = pltpu.make_async_copy(src, dst, sem.at[len(copies)])
        copy.start()
        copies.append(copy)

    for k in range(count):
        go(whole.at[pl.ds(k * step, step), pl.ds(0, cols)], codes_out.at[pl.ds(k * step, step), :])
    go(whole.at[:, pl.ds(cols, scales_out.shape[1])], scales_out)
    go(new_master, master_out)
    go(new_first, first_out)
    go(new_second, second_out)
    for copy in copies:
        copy.wait()


def per_device(master, gradient, first_moment, second_moment, max_norm, step_count):
    rows, width = master.shape
    cols = 2 * width
    scales = cols // BLOCK
    kept = 32 * rows
    full = cols + scales
    smem = pl.BlockSpec(memory_space=pltpu.SMEM)
    any_spec = pl.BlockSpec(memory_space=pl.ANY)
    vmem = pl.BlockSpec(memory_space=pltpu.VMEM)
    held = pl.pallas_call(
        gather_kernel,
        out_shape=tuple(pltpu.VMEM((rows, width), F32) for _ in range(3)) + (pltpu.VMEM((kept, full), BF16),),
        in_specs=[smem, smem] + [any_spec] * 4,
        out_specs=tuple(vmem for _ in range(4)),
        scratch_shapes=[
            pltpu.VMEM((4, rows, width), F32),
            pltpu.VMEM((4, rows, width), F32),
            pltpu.VMEM((PART, cols), F32),
            pltpu.VMEM((2, 4, PART, LANES), F32),
            pltpu.VMEM((3, 8, LANES), F32),
            pltpu.VMEM((13, 8, LANES), F32),
            pltpu.SemaphoreType.DMA((4,)),
            pltpu.SemaphoreType.DMA((2,)),
            pltpu.SemaphoreType.DMA((3,)),
            pltpu.SemaphoreType.DMA((3,)),
            pltpu.SemaphoreType.DMA((18,)),
            pltpu.SemaphoreType.DMA((SLOTS,)),
        ],
        compiler_params=pltpu.CompilerParams(collective_id=0, has_side_effects=True, vmem_limit_bytes=16 * 2**20),
        name="update_and_gather",
    )(
        max_norm,
        step_count,
        *(
            pltpu.with_memory_space_constraint(a, pltpu.HBM)
            for a in (master, gradient, first_moment, second_moment)
        ),
    )
    new_master, new_first, new_second, whole = (
        pltpu.with_memory_space_constraint(a, pltpu.VMEM) for a in held
    )
    codes, block_scales, new_master, new_first, new_second = pl.pallas_call(
        write_kernel,
        out_shape=(
            jax.ShapeDtypeStruct((kept, cols), BF16),
            jax.ShapeDtypeStruct((kept, scales), BF16),
        )
        + tuple(jax.ShapeDtypeStruct((rows, width), F32) for _ in range(3)),
        in_specs=[vmem] * 4,
        out_specs=tuple(any_spec for _ in range(5)),
        scratch_shapes=[pltpu.SemaphoreType.DMA((12,))],
        compiler_params=pltpu.CompilerParams(vmem_limit_bytes=16 * 2**20),
        name="write_results",
    )(whole, new_master, new_first, new_second)
    return (new_master, new_first, new_second, codes, block_scales)


def solution(mesh):
    return jax.shard_map(
        per_device,
        mesh=mesh,
        in_specs=(P("shard", "pair"),) * 4 + (P(), P()),
        out_specs=(P("shard", "pair"),) * 3 + (P("pair", None),) * 2,
        check_vma=False,
    )
```

```python
import functools
import heapq
import itertools

import jax
import jax.numpy as jnp
import numpy as np
from jax import lax
from jax.experimental import pallas as pl
from jax.experimental.pallas import tpu as pltpu
from jax.sharding import PartitionSpec as P

MESH = pl.DeviceIdType.MESH
F32, BF16 = jnp.float32, jnp.bfloat16

beta_first = 0.9
beta_second = 0.99
learn_rate = 0.01
decay_rate = 0.1
adam_eps = 1e-06
scale_floor = 0.25

BLOCK = 32
PART = 16
LANES = 128
ORDERS = ((0, 1, 2), (1, 2, 0), (2, 0, 1))


def hops(part, plane, off):
    order = ORDERS[part]
    last = max([j for j, d in enumerate(order) if off[d]], default=-1)
    out = []
    if last >= 0:
        d = order[last]
        swap = d == 2 and plane == 1
        if off[d] == 1:
            out.append((d, 1, 2 if swap else 1))
        if off[d] == 3:
            out.append((d, -1, 1 if swap else 2))
    for d in order[last + 1 :]:
        out += [(d, 1, 0), (d, -1, 0)]
    return out


def arrivals(unit=1.45, latency=1.7, ready=(0.6, 1.2, 1.8)):
    queues = {(r, d, s): [] for r in range(4) for d in range(3) for s in (1, -1)}
    heads, events, count, now = {}, [], itertools.count(), 0.0
    got = {r: {} for r in range(4)}
    order = {r: [] for r in range(4)}
    for r in (0, 1):
        for p in range(3):
            heapq.heappush(events, (ready[p], next(count), r, (p, r, 0, 0), 0))
    while True:
        for k in queues:
            if k not in heads and queues[k]:
                item = queues[k].pop(0)
                heads[k] = [unit if item[1] == 0 else unit / 2, item]
        rate = {k: 0.5 if ((k[0] + 2) % 4, k[1], k[2]) in heads else 1.0 for k in heads}
        times = [now + heads[k][0] / rate[k] for k in heads] + ([events[0][0]] if events else [])
        if not times:
            return order
        then = min(times)
        for k in heads:
            heads[k][0] -= (then - now) * rate[k]
        now = then
        for k in list(heads):
            if heads[k][0] <= 1e-9:
                (r, d, s), ((p, plane, ox, oy), half) = k, heads.pop(k)[1]
                if d == 0:
                    ox = (ox + s) % 4
                elif d == 1:
                    oy = (oy + s) % 4
                else:
                    r = (r + s) % 4
                heapq.heappush(events, (now + latency, next(count), r, (p, plane, ox, oy), half))
        while events and events[0][0] <= now + 1e-9:
            _, _, r, chunk, half = heapq.heappop(events)
            p, plane, ox, oy = chunk
            off = (ox, oy, (r - plane) % 4)
            if off != (0, 0, 0):
                order[r].append((chunk, half))
            seen = got[r].setdefault(chunk, set())
            seen.add(half)
            if 0 in seen or len(seen) == 2:
                for d, s, h in hops(p, plane, off):
                    queues[(r, d, s)].append((chunk, h))


def is_leaf(role, chunk):
    p, plane, ox, oy = chunk
    return not hops(p, plane, (ox, oy, (role - plane) % 4))


SCHEDULE = arrivals()
SLOTS = {
    role: {piece: n for n, piece in enumerate(p for p in SCHEDULE[role] if not is_leaf(role, p[0]))}
    for role in (0, 3)
}
LEAVES = max(len(s) for s in SLOTS.values())


def slot(role, chunk, half):
    return LEAVES + (half == 2) if is_leaf(role, chunk) else SLOTS[role][(chunk, half)]


def gather_kernel(
    max_norm,
    step_count,
    master,
    gradient,
    first,
    second,
    new_master,
    new_first,
    new_second,
    whole,
    own,
    other,
    fresh,
    largest,
    sums,
    sum_rx,
    load_sem,
    swap_sem,
    sum_send,
    sum_recv,
    send_sem,
    recv_sem,
):
    rows, width = own.shape[1:]
    parts = rows // PART
    cols = 2 * width
    full = whole.shape[1]
    cut = LANES * ((full // LANES + 1) // 2)

    me = lax.axis_index("shard")
    core = lax.axis_index("pair")
    x, y, z = lax.rem(me, 4), lax.rem(lax.div(me, 4), 4), lax.div(me, 16)
    role = lax.rem(z + 2 * core, 4)
    source = role < 2
    flip = jnp.logical_or(role == 1, role == 2)
    sigma = jnp.where(flip, -1, 1)

    def at(xx, yy, zz):
        return lax.rem(zz, 4) * 16 + lax.rem(yy, 4) * 4 + lax.rem(xx, 4)

    partner = (1 - core, me)
    x_peers = [(k, at(x + dx, y, z)) for dx in (1, 2, 3) for k in (core, 1 - core)] + [partner]
    y_peers = [(core, at(x, y + d, z)) for d in (1, 2, 3)]
    z_peers = [(core, at(x, y, z + d)) for d in (1, 2, 3)]
    barrier = pltpu.get_barrier_semaphore()
    peers = x_peers + y_peers + z_peers
    for peer in peers:
        pl.semaphore_signal(barrier, inc=1, device_id=peer, device_id_type=MESH)

    loads = [
        pltpu.make_async_copy(ref, own.at[k], load_sem.at[k])
        for k, ref in enumerate((gradient, first, second, master))
    ]
    for load in loads:
        load.start()
    loads[0].wait()
    acc = jnp.zeros((8, LANES), F32)
    for i in range(0, rows, 8):
        for j in range(0, width, LANES):
            g = own[0, i : i + 8, j : j + LANES]
            acc = acc + g * g
    sums[0] = acc
    for load in loads[1:]:
        load.wait()
    pl.semaphore_wait(barrier, len(peers))

    def exchange(step, base, to):
        copies = [
            pltpu.make_async_remote_copy(
                src_ref=sums.at[step],
                dst_ref=sum_rx.at[base + k],
                send_sem=sum_send.at[step],
                recv_sem=sum_recv.at[step],
                device_id=peer,
                device_id_type=MESH,
            )
            for k, peer in enumerate(to)
        ]
        for copy in copies:
            copy.start()
        slots = sum_rx.at[pl.ds(base, len(to))]
        return pltpu.make_async_remote_copy(
            src_ref=slots,
            dst_ref=slots,
            send_sem=sum_send.at[step],
            recv_sem=sum_recv.at[step],
            device_id=to[0],
            device_id_type=MESH,
        )

    swap = pltpu.make_async_remote_copy(
        src_ref=own,
        dst_ref=other,
        send_sem=swap_sem.at[0],
        recv_sem=swap_sem.at[1],
        device_id=partner,
        device_id_type=MESH,
    )

    exchanges = []
    base = 0
    for step, to in enumerate((x_peers, y_peers, z_peers)):
        started = exchange(step, base, to)
        if step == 0:

            @pl.when(jnp.logical_not(source))
            def _():
                swap.start()

        started.wait_recv()
        acc = sums[step]
        for k in range(len(to)):
            acc = acc + sum_rx[base + k]
        base += len(to)
        exchanges.append(started)
        if step < 2:
            sums[step + 1] = acc

    squares = jnp.sum(acc, axis=(0, 1), keepdims=True)
    limit = jnp.full((1, 1), max_norm[0], F32)
    clip = limit / jnp.maximum(jnp.sqrt(squares), limit)
    counted = jnp.full((1, 1), step_count[0], jnp.int32).astype(F32)
    inv_first = 1.0 / (1.0 - jnp.exp(counted * float(np.log(beta_first))))
    inv_second = 1.0 / (1.0 - jnp.exp(counted * float(np.log(beta_second))))
    clip = jnp.broadcast_to(clip, (PART, LANES))
    inv_first = jnp.broadcast_to(inv_first, (PART, LANES))
    inv_second = jnp.broadcast_to(inv_second, (PART, LANES))

    lane = lax.broadcasted_iota(jnp.int32, (PART, LANES), 1)
    block_start = lane - lax.bitwise_and(lane, BLOCK - 1)
    to_lane = lax.broadcasted_iota(jnp.int32, (LANES, LANES), 1)
    from_lane = lax.broadcasted_iota(jnp.int32, (LANES, LANES), 0)
    spread = jnp.where(
        lax.div(from_lane, BLOCK) + (LANES // BLOCK) * lax.rem(from_lane, BLOCK) == to_lane, 1.0, 0.0
    ).astype(BF16)

    def adam(held, i, j):
        g, m, v, w = (held[k, pl.ds(i, PART), pl.ds(j, LANES)] for k in range(4))
        clipped = clip * g
        m = beta_first * m + (1.0 - beta_first) * clipped
        v = beta_second * v + (1.0 - beta_second) * clipped * clipped
        update = m * inv_first / (jnp.sqrt(v * inv_second) + adam_eps) + decay_rate * w
        return w - learn_rate * update, m, v

    tiles = width // LANES
    step_tiles = 4

    def store(i, j, w, m, v):
        new_master[pl.ds(i, PART), pl.ds(j, LANES)] = w
        new_first[pl.ds(i, PART), pl.ds(j, LANES)] = m
        new_second[pl.ds(i, PART), pl.ds(j, LANES)] = v

    def merge(a, b, bit):
        here = lax.bitwise_and(lane, bit) != 0
        crossed = jnp.where(here, a, b)
        crossed = jnp.where(here, pltpu.roll(crossed, bit, 1), pltpu.roll(crossed, LANES - bit, 1))
        return jnp.maximum(jnp.where(here, b, a), crossed)

    def merge_all(values, bit):
        while len(values) > 1:
            values = [merge(a, b, bit) for a, b in zip(values[::2], values[1::2])]
            bit *= 2
        return values[0]

    def update_chunk(i, row):
        def update(t, carry):
            for half, held in enumerate((own, other)):
                at_half = core if half == 0 else 1 - core
                sizes = []
                for k in range(step_tiles):
                    j = pl.multiple_of((t * step_tiles + k) * LANES, LANES)
                    w, m, v = adam(held, i, j)
                    if half == 0:
                        store(i, j, w, m, v)
                    fresh[:, pl.ds(pl.multiple_of(at_half * width + j, LANES), LANES)] = w
                    sizes.append(jnp.abs(w))
                largest[half, t] = merge_all(sizes, 1)
            return carry

        lax.fori_loop(0, tiles // step_tiles, update, 0)
        mine, others = (merge_all([largest[h, t] for t in range(tiles // step_tiles)], step_tiles) for h in (0, 1))
        top = merge(jnp.where(core == 0, mine, others), jnp.where(core == 0, others, mine), tiles)
        scales = jnp.maximum(top, scale_floor).astype(BF16)
        whole[pl.ds(row, PART), cols:] = jnp.dot(scales, spread, preferred_element_type=F32).astype(BF16)
        inverse = 1.0 / scales.astype(F32)

        def code(t, carry):
            for k in range(2 * step_tiles):
                tile = t * 2 * step_tiles + k
                j = pl.ds(pl.multiple_of(tile * LANES, LANES), LANES)
                by = jnp.take_along_axis(inverse, block_start + tile, axis=1, mode="promise_in_bounds")
                whole[pl.ds(row, PART), j] = (fresh[:, j] * by).astype(BF16)
            return carry

        lax.fori_loop(0, tiles // step_tiles, code, 0)

    line = [[(lax.rem(y + 4 - oy, 4) * 4 + lax.rem(x + 4 - ox, 4)) * rows for oy in range(4)] for ox in range(4)]
    plane_row = [jnp.where(flip, 16 * rows, 0), jnp.where(flip, 0, 16 * rows)]
    near = {
        (0, 1): at(x + 1, y, z),
        (0, -1): at(x + 3, y, z),
        (1, 1): at(x, y + 1, z),
        (1, -1): at(x, y + 3, z),
        (2, 1): at(x, y, z + 4 + sigma),
        (2, -1): at(x, y, z + 4 - sigma),
    }
    pieces = {0: pl.ds(0, full), 1: pl.ds(0, cut), 2: pl.ds(cut, full - cut)}

    def place(chunk, half):
        p, plane, ox, oy = chunk
        return whole.at[pl.ds(pl.multiple_of(line[ox][oy] + plane_row[plane] + p * PART, PART), PART), pieces[half]]

    def lane_of(d, s, half):
        return (d * 2 + (s < 0)) * 3 + half

    def piece(chunk, half, role_now, d, s):
        p, plane, ox, oy = chunk
        role = role_now
        if d == 0:
            ox = (ox + s) % 4
        elif d == 1:
            oy = (oy + s) % 4
        elif (role_now == 0) == (s == 1):
            plane = 1 - plane
        else:
            role = 3 - role_now
        ref = place(chunk, half)
        return pltpu.make_async_remote_copy(
            src_ref=ref,
            dst_ref=ref,
            send_sem=send_sem.at[lane_of(d, s, half)],
            recv_sem=recv_sem.at[slot(role, (p, plane, ox, oy), half)],
            device_id=(core, near[(d, s)]),
            device_id_type=MESH,
        )

    def landed(number, ref):
        pltpu.make_async_remote_copy(
            src_ref=ref,
            dst_ref=ref,
            send_sem=send_sem.at[0],
            recv_sem=recv_sem.at[number],
            device_id=(core, near[(0, 1)]),
            device_id_type=MESH,
        ).wait_recv()

    def follow(role_now, order, sent):
        got = {}
        leaves = [h for chunk, h in order if is_leaf(role_now, chunk)]
        for chunk, half in order:
            if is_leaf(role_now, chunk):
                continue
            landed(slot(role_now, chunk, half), place(chunk, half))
            seen = got.setdefault(chunk, set())
            seen.add(half)
            if 0 in seen or len(seen) == 2:
                p, plane, ox, oy = chunk
                for d, s, h in hops(p, plane, (ox, oy, (role_now - plane) % 4)):
                    piece(chunk, h, role_now, d, s).start()
                    sent.append((d, s, h))
        for h in sorted(set(leaves)):
            landed(LEAVES + (h == 2), whole.at[pl.ds(0, PART * leaves.count(h)), pieces[h]])
        for d, s, h in sorted(set(sent)):
            total = whole.at[pl.ds(0, PART * sent.count((d, s, h))), pieces[h]]
            pltpu.make_async_remote_copy(
                src_ref=total,
                dst_ref=total,
                send_sem=send_sem.at[lane_of(d, s, h)],
                recv_sem=recv_sem.at[0],
                device_id=(core, near[(d, s)]),
                device_id_type=MESH,
            ).wait_send()

    @pl.when(source)
    def _():
        swap.wait_recv()
        sent = []
        for p in range(parts):
            i = p * PART
            row = pl.multiple_of(line[0][0] + plane_row[0] + i, PART)

            update_chunk(i, row)
            for d, s, h in hops(p, 0, (0, 0, 0)):
                piece((p, 0, 0, 0), h, 0, d, s).start()
                sent.append((d, s, h))
        follow(0, SCHEDULE[0], sent)

    @pl.when(jnp.logical_not(source))
    def _():
        for p in range(parts):
            i = p * PART

            def body(t, carry, i=i):
                for k in range(step_tiles):
                    j = pl.multiple_of((t * step_tiles + k) * LANES, LANES)
                    store(i, j, *adam(own, i, j))
                return carry

            lax.fori_loop(0, tiles // step_tiles, body, 0)
        follow(3, SCHEDULE[3], [])
        swap.wait_send()

    for started in exchanges:
        started.wait_send()


def write_kernel(whole, new_master, new_first, new_second, codes_out, scales_out, master_out, first_out, second_out, sem):
    rows, cols = codes_out.shape
    count = 8
    step = rows // count
    copies = []

    def go(src, dst):
        copy = pltpu.make_async_copy(src, dst, sem.at[len(copies)])
        copy.start()
        copies.append(copy)

    for k in range(count):
        go(whole.at[pl.ds(k * step, step), pl.ds(0, cols)], codes_out.at[pl.ds(k * step, step), :])
    go(whole.at[:, pl.ds(cols, scales_out.shape[1])], scales_out)
    go(new_master, master_out)
    go(new_first, first_out)
    go(new_second, second_out)
    for copy in copies:
        copy.wait()


def per_device(master, gradient, first_moment, second_moment, max_norm, step_count):
    rows, width = master.shape
    cols = 2 * width
    scales = cols // BLOCK
    kept = 32 * rows
    full = cols + scales
    smem = pl.BlockSpec(memory_space=pltpu.SMEM)
    any_spec = pl.BlockSpec(memory_space=pl.ANY)
    vmem = pl.BlockSpec(memory_space=pltpu.VMEM)
    held = pl.pallas_call(
        gather_kernel,
        out_shape=tuple(pltpu.VMEM((rows, width), F32) for _ in range(3)) + (pltpu.VMEM((kept, full), BF16),),
        in_specs=[smem, smem] + [any_spec] * 4,
        out_specs=tuple(vmem for _ in range(4)),
        scratch_shapes=[
            pltpu.VMEM((4, rows, width), F32),
            pltpu.VMEM((4, rows, width), F32),
            pltpu.VMEM((PART, cols), F32),
            pltpu.VMEM((2, 4, PART, LANES), F32),
            pltpu.VMEM((3, 8, LANES), F32),
            pltpu.VMEM((13, 8, LANES), F32),
            pltpu.SemaphoreType.DMA((4,)),
            pltpu.SemaphoreType.DMA((2,)),
            pltpu.SemaphoreType.DMA((3,)),
            pltpu.SemaphoreType.DMA((3,)),
            pltpu.SemaphoreType.DMA((18,)),
            pltpu.SemaphoreType.DMA((LEAVES + 2,)),
        ],
        compiler_params=pltpu.CompilerParams(collective_id=0, has_side_effects=True, vmem_limit_bytes=16 * 2**20),
        name="update_and_gather",
    )(
        max_norm,
        step_count,
        *(
            pltpu.with_memory_space_constraint(a, pltpu.HBM)
            for a in (master, gradient, first_moment, second_moment)
        ),
    )
    new_master, new_first, new_second, whole = (
        pltpu.with_memory_space_constraint(a, pltpu.VMEM) for a in held
    )
    codes, block_scales, new_master, new_first, new_second = pl.pallas_call(
        write_kernel,
        out_shape=(
            jax.ShapeDtypeStruct((kept, cols), BF16),
            jax.ShapeDtypeStruct((kept, scales), BF16),
        )
        + tuple(jax.ShapeDtypeStruct((rows, width), F32) for _ in range(3)),
        in_specs=[vmem] * 4,
        out_specs=tuple(any_spec for _ in range(5)),
        scratch_shapes=[pltpu.SemaphoreType.DMA((12,))],
        compiler_params=pltpu.CompilerParams(vmem_limit_bytes=16 * 2**20),
        name="write_results",
    )(whole, new_master, new_first, new_second)
    return (new_master, new_first, new_second, codes, block_scales)


def solution(mesh):
    return jax.shard_map(
        per_device,
        mesh=mesh,
        in_specs=(P("shard", "pair"),) * 4 + (P(), P()),
        out_specs=(P("shard", "pair"),) * 3 + (P("pair", None),) * 2,
        check_vma=False,
    )
```

```python
import functools
import heapq
import itertools

import jax
import jax.numpy as jnp
import numpy as np
from jax import lax
from jax.experimental import pallas as pl
from jax.experimental.pallas import tpu as pltpu
from jax.sharding import PartitionSpec as P

MESH = pl.DeviceIdType.MESH
F32, BF16 = jnp.float32, jnp.bfloat16

beta_first = 0.9
beta_second = 0.99
learn_rate = 0.01
decay_rate = 0.1
adam_eps = 1e-06
scale_floor = 0.25

BLOCK = 32
PART = 16
LANES = 128
ORDERS = ((0, 1, 2), (1, 2, 0), (2, 0, 1))


def hops(part, plane, off):
    order = ORDERS[part]
    last = max([j for j, d in enumerate(order) if off[d]], default=-1)
    out = []
    if last >= 0:
        d = order[last]
        swap = d == 2 and plane == 1
        if off[d] == 1:
            out.append((d, 1, 2 if swap else 1))
        if off[d] == 3:
            out.append((d, -1, 1 if swap else 2))
    for d in order[last + 1 :]:
        out += [(d, 1, 0), (d, -1, 0)]
    return out


def arrivals(unit=1.45, latency=1.7, ready=(0.6, 1.2, 1.8)):
    queues = {(r, d, s): [] for r in range(4) for d in range(3) for s in (1, -1)}
    heads, events, count, now = {}, [], itertools.count(), 0.0
    got = {r: {} for r in range(4)}
    order = {r: [] for r in range(4)}
    for r in (0, 1):
        for p in range(3):
            heapq.heappush(events, (ready[p], next(count), r, (p, r, 0, 0), 0))
    while True:
        for k in queues:
            if k not in heads and queues[k]:
                item = queues[k].pop(0)
                heads[k] = [unit if item[1] == 0 else unit / 2, item]
        rate = {k: 0.5 if ((k[0] + 2) % 4, k[1], k[2]) in heads else 1.0 for k in heads}
        times = [now + heads[k][0] / rate[k] for k in heads] + ([events[0][0]] if events else [])
        if not times:
            return order
        then = min(times)
        for k in heads:
            heads[k][0] -= (then - now) * rate[k]
        now = then
        for k in list(heads):
            if heads[k][0] <= 1e-9:
                (r, d, s), ((p, plane, ox, oy), half) = k, heads.pop(k)[1]
                if d == 0:
                    ox = (ox + s) % 4
                elif d == 1:
                    oy = (oy + s) % 4
                else:
                    r = (r + s) % 4
                heapq.heappush(events, (now + latency, next(count), r, (p, plane, ox, oy), half))
        while events and events[0][0] <= now + 1e-9:
            _, _, r, chunk, half = heapq.heappop(events)
            p, plane, ox, oy = chunk
            off = (ox, oy, (r - plane) % 4)
            if off != (0, 0, 0):
                order[r].append((chunk, half))
            seen = got[r].setdefault(chunk, set())
            seen.add(half)
            if 0 in seen or len(seen) == 2:
                for d, s, h in hops(p, plane, off):
                    queues[(r, d, s)].append((chunk, h))


def is_leaf(role, chunk):
    p, plane, ox, oy = chunk
    return not hops(p, plane, (ox, oy, (role - plane) % 4))


SCHEDULE = arrivals()
SLOTS = {
    role: {piece: n for n, piece in enumerate(p for p in SCHEDULE[role] if not is_leaf(role, p[0]))}
    for role in (0, 3)
}
LEAVES = max(len(s) for s in SLOTS.values())


def slot(role, chunk, half):
    return LEAVES + (half == 2) if is_leaf(role, chunk) else SLOTS[role][(chunk, half)]


def gather_kernel(
    max_norm,
    step_count,
    master,
    gradient,
    first,
    second,
    new_master,
    new_first,
    new_second,
    whole,
    own,
    other,
    fresh,
    largest,
    sums,
    sum_rx,
    load_sem,
    swap_sem,
    sum_send,
    sum_recv,
    send_sem,
    recv_sem,
):
    rows, width = own.shape[1:]
    parts = rows // PART
    cols = 2 * width
    full = whole.shape[1]
    cut = LANES * ((full // LANES + 1) // 2)

    me = lax.axis_index("shard")
    core = lax.axis_index("pair")
    x, y, z = lax.rem(me, 4), lax.rem(lax.div(me, 4), 4), lax.div(me, 16)
    role = lax.rem(z + 2 * core, 4)
    source = role < 2
    flip = jnp.logical_or(role == 1, role == 2)
    sigma = jnp.where(flip, -1, 1)

    def at(xx, yy, zz):
        return lax.rem(zz, 4) * 16 + lax.rem(yy, 4) * 4 + lax.rem(xx, 4)

    partner = (1 - core, me)
    plane_peers = [(core, at(x + dx, y + dy, z)) for dx in (2, 1, 3, 0) for dy in (2, 1, 3, 0) if dx or dy]
    line_peers = [(k, at(x, y, z + d)) for d in (2, 1, 3) for k in (1 - core, core)] + [partner]
    barrier = pltpu.get_barrier_semaphore()
    peers = plane_peers + line_peers
    for peer in peers:
        pl.semaphore_signal(barrier, inc=1, device_id=peer, device_id_type=MESH)

    loads = [
        pltpu.make_async_copy(ref, own.at[k], load_sem.at[k])
        for k, ref in enumerate((gradient, first, second, master))
    ]
    for load in loads:
        load.start()
    loads[0].wait()
    acc = jnp.zeros((8, LANES), F32)
    for i in range(0, rows, 8):
        for j in range(0, width, LANES):
            g = own[0, i : i + 8, j : j + LANES]
            acc = acc + g * g
    sums[0] = jnp.sum(acc, axis=0, keepdims=True)
    for load in loads[1:]:
        load.wait()
    pl.semaphore_wait(barrier, len(peers))

    def exchange(step, base, to):
        copies = [
            pltpu.make_async_remote_copy(
                src_ref=sums.at[step],
                dst_ref=sum_rx.at[base + k],
                send_sem=sum_send.at[step],
                recv_sem=sum_recv.at[step],
                device_id=peer,
                device_id_type=MESH,
            )
            for k, peer in enumerate(to)
        ]
        for copy in copies:
            copy.start()
        slots = sum_rx.at[pl.ds(base, len(to))]
        return pltpu.make_async_remote_copy(
            src_ref=slots,
            dst_ref=slots,
            send_sem=sum_send.at[step],
            recv_sem=sum_recv.at[step],
            device_id=to[0],
            device_id_type=MESH,
        )

    swap = pltpu.make_async_remote_copy(
        src_ref=own,
        dst_ref=other,
        send_sem=swap_sem.at[0],
        recv_sem=swap_sem.at[1],
        device_id=partner,
        device_id_type=MESH,
    )

    exchanges = []
    base = 0
    for step, to in enumerate((plane_peers, line_peers)):
        started = exchange(step, base, to)
        if step == 0:

            @pl.when(jnp.logical_not(source))
            def _():
                swap.start()

        started.wait_recv()
        acc = sums[step]
        for k in range(len(to)):
            acc = acc + sum_rx[base + k]
        base += len(to)
        exchanges.append(started)
        if step < 1:
            sums[step + 1] = acc

    squares = jnp.sum(acc, axis=(0, 1), keepdims=True)
    limit = jnp.full((1, 1), max_norm[0], F32)
    clip = limit / jnp.maximum(jnp.sqrt(squares), limit)
    counted = jnp.full((1, 1), step_count[0], jnp.int32).astype(F32)
    inv_first = 1.0 / (1.0 - jnp.exp(counted * float(np.log(beta_first))))
    inv_second = 1.0 / (1.0 - jnp.exp(counted * float(np.log(beta_second))))
    clip = jnp.broadcast_to(clip, (PART, LANES))
    inv_first = jnp.broadcast_to(inv_first, (PART, LANES))
    inv_second = jnp.broadcast_to(inv_second, (PART, LANES))

    lane = lax.broadcasted_iota(jnp.int32, (PART, LANES), 1)
    block_start = lane - lax.bitwise_and(lane, BLOCK - 1)
    to_lane = lax.broadcasted_iota(jnp.int32, (LANES, LANES), 1)
    from_lane = lax.broadcasted_iota(jnp.int32, (LANES, LANES), 0)
    spread = jnp.where(
        lax.div(from_lane, BLOCK) + (LANES // BLOCK) * lax.rem(from_lane, BLOCK) == to_lane, 1.0, 0.0
    ).astype(BF16)

    def adam(held, i, j):
        g, m, v, w = (held[k, pl.ds(i, PART), pl.ds(j, LANES)] for k in range(4))
        clipped = clip * g
        m = beta_first * m + (1.0 - beta_first) * clipped
        v = beta_second * v + (1.0 - beta_second) * clipped * clipped
        update = m * inv_first / (jnp.sqrt(v * inv_second) + adam_eps) + decay_rate * w
        return w - learn_rate * update, m, v

    tiles = width // LANES
    step_tiles = 4

    def store(i, j, w, m, v):
        new_master[pl.ds(i, PART), pl.ds(j, LANES)] = w
        new_first[pl.ds(i, PART), pl.ds(j, LANES)] = m
        new_second[pl.ds(i, PART), pl.ds(j, LANES)] = v

    def merge(a, b, bit):
        here = lax.bitwise_and(lane, bit) != 0
        crossed = jnp.where(here, a, b)
        crossed = jnp.where(here, pltpu.roll(crossed, bit, 1), pltpu.roll(crossed, LANES - bit, 1))
        return jnp.maximum(jnp.where(here, b, a), crossed)

    def merge_all(values, bit):
        while len(values) > 1:
            values = [merge(a, b, bit) for a, b in zip(values[::2], values[1::2])]
            bit *= 2
        return values[0]

    def update_chunk(i, row):
        def update(t, carry):
            for half, held in enumerate((own, other)):
                at_half = core if half == 0 else 1 - core
                sizes = []
                for k in range(step_tiles):
                    j = pl.multiple_of((t * step_tiles + k) * LANES, LANES)
                    w, m, v = adam(held, i, j)
                    if half == 0:
                        store(i, j, w, m, v)
                    fresh[:, pl.ds(pl.multiple_of(at_half * width + j, LANES), LANES)] = w
                    sizes.append(jnp.abs(w))
                largest[half, t] = merge_all(sizes, 1)
            return carry

        lax.fori_loop(0, tiles // step_tiles, update, 0)
        mine, others = (merge_all([largest[h, t] for t in range(tiles // step_tiles)], step_tiles) for h in (0, 1))
        top = merge(jnp.where(core == 0, mine, others), jnp.where(core == 0, others, mine), tiles)
        scales = jnp.maximum(top, scale_floor).astype(BF16)
        whole[pl.ds(row, PART), cols:] = jnp.dot(scales, spread, preferred_element_type=F32).astype(BF16)
        inverse = 1.0 / scales.astype(F32)

        def code(t, carry):
            for k in range(2 * step_tiles):
                tile = t * 2 * step_tiles + k
                j = pl.ds(pl.multiple_of(tile * LANES, LANES), LANES)
                by = jnp.take_along_axis(inverse, block_start + tile, axis=1, mode="promise_in_bounds")
                whole[pl.ds(row, PART), j] = (fresh[:, j] * by).astype(BF16)
            return carry

        lax.fori_loop(0, tiles // step_tiles, code, 0)

    line = [[(lax.rem(y + 4 - oy, 4) * 4 + lax.rem(x + 4 - ox, 4)) * rows for oy in range(4)] for ox in range(4)]
    plane_row = [jnp.where(flip, 16 * rows, 0), jnp.where(flip, 0, 16 * rows)]
    near = {
        (0, 1): at(x + 1, y, z),
        (0, -1): at(x + 3, y, z),
        (1, 1): at(x, y + 1, z),
        (1, -1): at(x, y + 3, z),
        (2, 1): at(x, y, z + 4 + sigma),
        (2, -1): at(x, y, z + 4 - sigma),
    }
    pieces = {0: pl.ds(0, full), 1: pl.ds(0, cut), 2: pl.ds(cut, full - cut)}

    def place(chunk, half):
        p, plane, ox, oy = chunk
        return whole.at[pl.ds(pl.multiple_of(line[ox][oy] + plane_row[plane] + p * PART, PART), PART), pieces[half]]

    def lane_of(d, s, half):
        return (d * 2 + (s < 0)) * 3 + half

    def piece(chunk, half, role_now, d, s):
        p, plane, ox, oy = chunk
        role = role_now
        if d == 0:
            ox = (ox + s) % 4
        elif d == 1:
            oy = (oy + s) % 4
        elif (role_now == 0) == (s == 1):
            plane = 1 - plane
        else:
            role = 3 - role_now
        ref = place(chunk, half)
        return pltpu.make_async_remote_copy(
            src_ref=ref,
            dst_ref=ref,
            send_sem=send_sem.at[lane_of(d, s, half)],
            recv_sem=recv_sem.at[slot(role, (p, plane, ox, oy), half)],
            device_id=(core, near[(d, s)]),
            device_id_type=MESH,
        )

    def landed(number, ref):
        pltpu.make_async_remote_copy(
            src_ref=ref,
            dst_ref=ref,
            send_sem=send_sem.at[0],
            recv_sem=recv_sem.at[number],
            device_id=(core, near[(0, 1)]),
            device_id_type=MESH,
        ).wait_recv()

    def follow(role_now, order, sent):
        got = {}
        leaves = [h for chunk, h in order if is_leaf(role_now, chunk)]
        for chunk, half in order:
            if is_leaf(role_now, chunk):
                continue
            landed(slot(role_now, chunk, half), place(chunk, half))
            seen = got.setdefault(chunk, set())
            seen.add(half)
            if 0 in seen or len(seen) == 2:
                p, plane, ox, oy = chunk
                for d, s, h in hops(p, plane, (ox, oy, (role_now - plane) % 4)):
                    piece(chunk, h, role_now, d, s).start()
                    sent.append((d, s, h))
        for h in sorted(set(leaves)):
            landed(LEAVES + (h == 2), whole.at[pl.ds(0, PART * leaves.count(h)), pieces[h]])
        for d, s, h in sorted(set(sent)):
            total = whole.at[pl.ds(0, PART * sent.count((d, s, h))), pieces[h]]
            pltpu.make_async_remote_copy(
                src_ref=total,
                dst_ref=total,
                send_sem=send_sem.at[lane_of(d, s, h)],
                recv_sem=recv_sem.at[0],
                device_id=(core, near[(d, s)]),
                device_id_type=MESH,
            ).wait_send()

    @pl.when(source)
    def _():
        swap.wait_recv()
        sent = []
        for p in range(parts):
            i = p * PART
            row = pl.multiple_of(line[0][0] + plane_row[0] + i, PART)

            update_chunk(i, row)
            for d, s, h in hops(p, 0, (0, 0, 0)):
                piece((p, 0, 0, 0), h, 0, d, s).start()
                sent.append((d, s, h))
        follow(0, SCHEDULE[0], sent)

    @pl.when(jnp.logical_not(source))
    def _():
        for p in range(parts):
            i = p * PART

            def body(t, carry, i=i):
                for k in range(step_tiles):
                    j = pl.multiple_of((t * step_tiles + k) * LANES, LANES)
                    store(i, j, *adam(own, i, j))
                return carry

            lax.fori_loop(0, tiles // step_tiles, body, 0)
        follow(3, SCHEDULE[3], [])
        swap.wait_send()

    for started in exchanges:
        started.wait_send()


def write_kernel(whole, new_master, new_first, new_second, codes_out, scales_out, master_out, first_out, second_out, sem):
    rows, cols = codes_out.shape
    count = 8
    step = rows // count
    copies = []

    def go(src, dst):
        copy = pltpu.make_async_copy(src, dst, sem.at[len(copies)])
        copy.start()
        copies.append(copy)

    for k in range(count):
        go(whole.at[pl.ds(k * step, step), pl.ds(0, cols)], codes_out.at[pl.ds(k * step, step), :])
    go(whole.at[:, pl.ds(cols, scales_out.shape[1])], scales_out)
    go(new_master, master_out)
    go(new_first, first_out)
    go(new_second, second_out)
    for copy in copies:
        copy.wait()


def per_device(master, gradient, first_moment, second_moment, max_norm, step_count):
    rows, width = master.shape
    cols = 2 * width
    scales = cols // BLOCK
    kept = 32 * rows
    full = cols + scales
    smem = pl.BlockSpec(memory_space=pltpu.SMEM)
    any_spec = pl.BlockSpec(memory_space=pl.ANY)
    vmem = pl.BlockSpec(memory_space=pltpu.VMEM)
    held = pl.pallas_call(
        gather_kernel,
        out_shape=tuple(pltpu.VMEM((rows, width), F32) for _ in range(3)) + (pltpu.VMEM((kept, full), BF16),),
        in_specs=[smem, smem] + [any_spec] * 4,
        out_specs=tuple(vmem for _ in range(4)),
        scratch_shapes=[
            pltpu.VMEM((4, rows, width), F32),
            pltpu.VMEM((4, rows, width), F32),
            pltpu.VMEM((PART, cols), F32),
            pltpu.VMEM((2, 4, PART, LANES), F32),
            pltpu.VMEM((2, 1, LANES), F32),
            pltpu.VMEM((22, 1, LANES), F32),
            pltpu.SemaphoreType.DMA((4,)),
            pltpu.SemaphoreType.DMA((2,)),
            pltpu.SemaphoreType.DMA((2,)),
            pltpu.SemaphoreType.DMA((2,)),
            pltpu.SemaphoreType.DMA((18,)),
            pltpu.SemaphoreType.DMA((LEAVES + 2,)),
        ],
        compiler_params=pltpu.CompilerParams(collective_id=0, has_side_effects=True, vmem_limit_bytes=16 * 2**20),
        name="update_and_gather",
    )(
        max_norm,
        step_count,
        *(
            pltpu.with_memory_space_constraint(a, pltpu.HBM)
            for a in (master, gradient, first_moment, second_moment)
        ),
    )
    new_master, new_first, new_second, whole = (
        pltpu.with_memory_space_constraint(a, pltpu.VMEM) for a in held
    )
    codes, block_scales, new_master, new_first, new_second = pl.pallas_call(
        write_kernel,
        out_shape=(
            jax.ShapeDtypeStruct((kept, cols), BF16),
            jax.ShapeDtypeStruct((kept, scales), BF16),
        )
        + tuple(jax.ShapeDtypeStruct((rows, width), F32) for _ in range(3)),
        in_specs=[vmem] * 4,
        out_specs=tuple(any_spec for _ in range(5)),
        scratch_shapes=[pltpu.SemaphoreType.DMA((12,))],
        compiler_params=pltpu.CompilerParams(vmem_limit_bytes=16 * 2**20),
        name="write_results",
    )(whole, new_master, new_first, new_second)
    return (new_master, new_first, new_second, codes, block_scales)


def solution(mesh):
    return jax.shard_map(
        per_device,
        mesh=mesh,
        in_specs=(P("shard", "pair"),) * 4 + (P(), P()),
        out_specs=(P("shard", "pair"),) * 3 + (P("pair", None),) * 2,
        check_vma=False,
    )
```

```python
import functools
import heapq
import itertools

import jax
import jax.numpy as jnp
import numpy as np
from jax import lax
from jax.experimental import pallas as pl
from jax.experimental.pallas import tpu as pltpu
from jax.sharding import PartitionSpec as P

MESH = pl.DeviceIdType.MESH
F32, BF16 = jnp.float32, jnp.bfloat16

beta_first = 0.9
beta_second = 0.99
learn_rate = 0.01
decay_rate = 0.1
adam_eps = 1e-06
scale_floor = 0.25

BLOCK = 32
PART = 16
LANES = 128
ORDERS = ((0, 1, 2), (1, 2, 0), (2, 0, 1))


def hops(part, plane, off):
    order = ORDERS[part]
    last = max([j for j, d in enumerate(order) if off[d]], default=-1)
    out = []
    if last >= 0:
        d = order[last]
        swap = d == 2 and plane == 1
        if off[d] == 1:
            out.append((d, 1, 2 if swap else 1))
        if off[d] == 3:
            out.append((d, -1, 1 if swap else 2))
    for d in order[last + 1 :]:
        out += [(d, 1, 0), (d, -1, 0)]
    return out


def arrivals(unit=1.5, latency=2.8, ready=(1.65, 3.3, 4.95)):
    queues = {(r, d, s): [] for r in range(4) for d in range(3) for s in (1, -1)}
    heads, events, count, now = {}, [], itertools.count(), 0.0
    got = {r: {} for r in range(4)}
    order = {r: [] for r in range(4)}
    for r in (0, 1):
        for p in range(3):
            heapq.heappush(events, (ready[p], next(count), r, (p, r, 0, 0), 0))
    while True:
        for k in queues:
            if k not in heads and queues[k]:
                item = queues[k].pop(0)
                heads[k] = [unit if item[1] == 0 else unit / 2, item]
        rate = {k: 0.5 if ((k[0] + 2) % 4, k[1], k[2]) in heads else 1.0 for k in heads}
        times = [now + heads[k][0] / rate[k] for k in heads] + ([events[0][0]] if events else [])
        if not times:
            return order
        then = min(times)
        for k in heads:
            heads[k][0] -= (then - now) * rate[k]
        now = then
        for k in list(heads):
            if heads[k][0] <= 1e-9:
                (r, d, s), ((p, plane, ox, oy), half) = k, heads.pop(k)[1]
                if d == 0:
                    ox = (ox + s) % 4
                elif d == 1:
                    oy = (oy + s) % 4
                else:
                    r = (r + s) % 4
                heapq.heappush(events, (now + latency, next(count), r, (p, plane, ox, oy), half))
        while events and events[0][0] <= now + 1e-9:
            _, _, r, chunk, half = heapq.heappop(events)
            p, plane, ox, oy = chunk
            off = (ox, oy, (r - plane) % 4)
            if off != (0, 0, 0):
                order[r].append((chunk, half))
            seen = got[r].setdefault(chunk, set())
            seen.add(half)
            if 0 in seen or len(seen) == 2:
                for d, s, h in hops(p, plane, off):
                    queues[(r, d, s)].append((chunk, h))


def is_leaf(role, chunk):
    p, plane, ox, oy = chunk
    return not hops(p, plane, (ox, oy, (role - plane) % 4))


SCHEDULE = arrivals()
SLOTS = {
    role: {piece: n for n, piece in enumerate(p for p in SCHEDULE[role] if not is_leaf(role, p[0]))}
    for role in (0, 3)
}
LEAVES = max(len(s) for s in SLOTS.values())


def slot(role, chunk, half):
    return LEAVES + (half == 2) if is_leaf(role, chunk) else SLOTS[role][(chunk, half)]


def gather_kernel(
    max_norm,
    step_count,
    master,
    gradient,
    first,
    second,
    new_master,
    new_first,
    new_second,
    whole,
    own,
    other,
    fresh,
    largest,
    sums,
    sum_rx,
    load_sem,
    swap_sem,
    sum_send,
    sum_recv,
    send_sem,
    recv_sem,
):
    rows, width = own.shape[1:]
    parts = rows // PART
    cols = 2 * width
    full = whole.shape[1]
    cut = LANES * ((full // LANES + 1) // 2)

    me = lax.axis_index("shard")
    core = lax.axis_index("pair")
    x, y, z = lax.rem(me, 4), lax.rem(lax.div(me, 4), 4), lax.div(me, 16)
    role = lax.rem(z + 2 * core, 4)
    source = role < 2
    flip = jnp.logical_or(role == 1, role == 2)
    sigma = jnp.where(flip, -1, 1)

    def at(xx, yy, zz):
        return lax.rem(zz, 4) * 16 + lax.rem(yy, 4) * 4 + lax.rem(xx, 4)

    partner = (1 - core, me)
    plane_peers = [(core, at(x + dx, y + dy, z)) for dx in (2, 1, 3, 0) for dy in (2, 1, 3, 0) if dx or dy]
    line_peers = [(k, at(x, y, z + d)) for d in (2, 1, 3) for k in (1 - core, core)] + [partner]
    barrier = pltpu.get_barrier_semaphore()
    peers = plane_peers + line_peers
    for peer in peers:
        pl.semaphore_signal(barrier, inc=1, device_id=peer, device_id_type=MESH)

    loads = [
        pltpu.make_async_copy(ref, own.at[k], load_sem.at[k])
        for k, ref in enumerate((gradient, first, second, master))
    ]
    for load in loads:
        load.start()
    loads[0].wait()
    acc = jnp.zeros((8, LANES), F32)
    for i in range(0, rows, 8):
        for j in range(0, width, LANES):
            g = own[0, i : i + 8, j : j + LANES]
            acc = acc + g * g
    sums[0] = jnp.sum(acc, axis=0, keepdims=True)
    for load in loads[1:]:
        load.wait()
    pl.semaphore_wait(barrier, len(peers))

    def exchange(step, base, to):
        copies = [
            pltpu.make_async_remote_copy(
                src_ref=sums.at[step],
                dst_ref=sum_rx.at[base + k],
                send_sem=sum_send.at[step],
                recv_sem=sum_recv.at[step],
                device_id=peer,
                device_id_type=MESH,
            )
            for k, peer in enumerate(to)
        ]
        for copy in copies:
            copy.start()
        slots = sum_rx.at[pl.ds(base, len(to))]
        return pltpu.make_async_remote_copy(
            src_ref=slots,
            dst_ref=slots,
            send_sem=sum_send.at[step],
            recv_sem=sum_recv.at[step],
            device_id=to[0],
            device_id_type=MESH,
        )

    swap = pltpu.make_async_remote_copy(
        src_ref=own,
        dst_ref=other,
        send_sem=swap_sem.at[0],
        recv_sem=swap_sem.at[1],
        device_id=partner,
        device_id_type=MESH,
    )

    exchanges = []
    base = 0
    for step, to in enumerate((plane_peers, line_peers)):
        started = exchange(step, base, to)
        if step == 0:

            @pl.when(jnp.logical_not(source))
            def _():
                swap.start()

        started.wait_recv()
        acc = sums[step]
        for k in range(len(to)):
            acc = acc + sum_rx[base + k]
        base += len(to)
        exchanges.append(started)
        if step < 1:
            sums[step + 1] = acc

    squares = jnp.sum(acc, axis=(0, 1), keepdims=True)
    limit = jnp.full((1, 1), max_norm[0], F32)
    clip = limit / jnp.maximum(jnp.sqrt(squares), limit)
    counted = jnp.full((1, 1), step_count[0], jnp.int32).astype(F32)
    inv_first = 1.0 / (1.0 - jnp.exp(counted * float(np.log(beta_first))))
    inv_second = 1.0 / (1.0 - jnp.exp(counted * float(np.log(beta_second))))
    clip = jnp.broadcast_to(clip, (PART, LANES))
    inv_first = jnp.broadcast_to(inv_first, (PART, LANES))
    inv_second = jnp.broadcast_to(inv_second, (PART, LANES))

    lane = lax.broadcasted_iota(jnp.int32, (PART, LANES), 1)
    block_start = lane - lax.bitwise_and(lane, BLOCK - 1)
    per_tile = LANES // BLOCK
    gathered = BLOCK * lax.rem(lane, per_tile) + lax.div(lane, per_tile)

    def adam(held, i, j):
        g, m, v, w = (held[k, pl.ds(i, PART), pl.ds(j, LANES)] for k in range(4))
        clipped = clip * g
        m = beta_first * m + (1.0 - beta_first) * clipped
        v = beta_second * v + (1.0 - beta_second) * clipped * clipped
        update = m * inv_first / (jnp.sqrt(v * inv_second) + adam_eps) + decay_rate * w
        return w - learn_rate * update, m, v

    tiles = width // LANES
    step_tiles = 4

    def store(i, j, w, m, v):
        new_master[pl.ds(i, PART), pl.ds(j, LANES)] = w
        new_first[pl.ds(i, PART), pl.ds(j, LANES)] = m
        new_second[pl.ds(i, PART), pl.ds(j, LANES)] = v

    def merge(a, b, bit):
        here = lax.bitwise_and(lane, bit) != 0
        crossed = jnp.where(here, a, b)
        crossed = jnp.where(here, pltpu.roll(crossed, bit, 1), pltpu.roll(crossed, LANES - bit, 1))
        return jnp.maximum(jnp.where(here, b, a), crossed)

    def merge_all(values, bit):
        while len(values) > 1:
            values = [merge(a, b, bit) for a, b in zip(values[::2], values[1::2])]
            bit *= 2
        return values[0]

    def update_chunk(i, row):
        def update(t, carry):
            for half, held in enumerate((own, other)):
                at_half = core if half == 0 else 1 - core
                sizes = []
                for k in range(step_tiles):
                    j = pl.multiple_of((t * step_tiles + k) * LANES, LANES)
                    w, m, v = adam(held, i, j)
                    if half == 0:
                        store(i, j, w, m, v)
                    fresh[:, pl.ds(pl.multiple_of(at_half * width + j, LANES), LANES)] = w
                    sizes.append(jnp.abs(w))
                largest[half, t] = merge_all(sizes, 1)
            return carry

        lax.fori_loop(0, tiles // step_tiles, update, 0)
        mine, others = (merge_all([largest[h, t] for t in range(tiles // step_tiles)], step_tiles) for h in (0, 1))
        top = merge(jnp.where(core == 0, mine, others), jnp.where(core == 0, others, mine), tiles)
        scales = jnp.maximum(top, scale_floor).astype(BF16).astype(F32)
        inverse = 1.0 / scales
        in_order = jnp.take_along_axis(scales, gathered, axis=1, mode="promise_in_bounds")
        whole[pl.ds(row, PART), cols:] = in_order.astype(BF16)

        def code(t, carry):
            for k in range(2 * step_tiles):
                tile = t * 2 * step_tiles + k
                j = pl.ds(pl.multiple_of(tile * LANES, LANES), LANES)
                by = jnp.take_along_axis(inverse, block_start + tile, axis=1, mode="promise_in_bounds")
                whole[pl.ds(row, PART), j] = (fresh[:, j] * by).astype(BF16)
            return carry

        lax.fori_loop(0, tiles // step_tiles, code, 0)

    line = [[(lax.rem(y + 4 - oy, 4) * 4 + lax.rem(x + 4 - ox, 4)) * rows for oy in range(4)] for ox in range(4)]
    plane_row = [jnp.where(flip, 16 * rows, 0), jnp.where(flip, 0, 16 * rows)]
    near = {
        (0, 1): at(x + 1, y, z),
        (0, -1): at(x + 3, y, z),
        (1, 1): at(x, y + 1, z),
        (1, -1): at(x, y + 3, z),
        (2, 1): at(x, y, z + 4 + sigma),
        (2, -1): at(x, y, z + 4 - sigma),
    }
    pieces = {0: pl.ds(0, full), 1: pl.ds(0, cut), 2: pl.ds(cut, full - cut)}

    def place(chunk, half):
        p, plane, ox, oy = chunk
        return whole.at[pl.ds(pl.multiple_of(line[ox][oy] + plane_row[plane] + p * PART, PART), PART), pieces[half]]

    def lane_of(d, s, half):
        return (d * 2 + (s < 0)) * 3 + half

    def piece(chunk, half, role_now, d, s):
        p, plane, ox, oy = chunk
        role = role_now
        if d == 0:
            ox = (ox + s) % 4
        elif d == 1:
            oy = (oy + s) % 4
        elif (role_now == 0) == (s == 1):
            plane = 1 - plane
        else:
            role = 3 - role_now
        ref = place(chunk, half)
        return pltpu.make_async_remote_copy(
            src_ref=ref,
            dst_ref=ref,
            send_sem=send_sem.at[lane_of(d, s, half)],
            recv_sem=recv_sem.at[slot(role, (p, plane, ox, oy), half)],
            device_id=(core, near[(d, s)]),
            device_id_type=MESH,
        )

    def landed(number, ref):
        pltpu.make_async_remote_copy(
            src_ref=ref,
            dst_ref=ref,
            send_sem=send_sem.at[0],
            recv_sem=recv_sem.at[number],
            device_id=(core, near[(0, 1)]),
            device_id_type=MESH,
        ).wait_recv()

    def follow(role_now, order, sent):
        got = {}
        leaves = [h for chunk, h in order if is_leaf(role_now, chunk)]
        for chunk, half in order:
            if is_leaf(role_now, chunk):
                continue
            landed(slot(role_now, chunk, half), place(chunk, half))
            seen = got.setdefault(chunk, set())
            seen.add(half)
            if 0 in seen or len(seen) == 2:
                p, plane, ox, oy = chunk
                for d, s, h in hops(p, plane, (ox, oy, (role_now - plane) % 4)):
                    piece(chunk, h, role_now, d, s).start()
                    sent.append((d, s, h))
        for h in sorted(set(leaves)):
            landed(LEAVES + (h == 2), whole.at[pl.ds(0, PART * leaves.count(h)), pieces[h]])
        for d, s, h in sorted(set(sent)):
            total = whole.at[pl.ds(0, PART * sent.count((d, s, h))), pieces[h]]
            pltpu.make_async_remote_copy(
                src_ref=total,
                dst_ref=total,
                send_sem=send_sem.at[lane_of(d, s, h)],
                recv_sem=recv_sem.at[0],
                device_id=(core, near[(d, s)]),
                device_id_type=MESH,
            ).wait_send()

    @pl.when(source)
    def _():
        swap.wait_recv()
        sent = []
        for p in range(parts):
            i = p * PART
            row = pl.multiple_of(line[0][0] + plane_row[0] + i, PART)

            update_chunk(i, row)
            for d, s, h in hops(p, 0, (0, 0, 0)):
                piece((p, 0, 0, 0), h, 0, d, s).start()
                sent.append((d, s, h))
        follow(0, SCHEDULE[0], sent)

    @pl.when(jnp.logical_not(source))
    def _():
        for p in range(parts):
            i = p * PART

            def body(t, carry, i=i):
                for k in range(step_tiles):
                    j = pl.multiple_of((t * step_tiles + k) * LANES, LANES)
                    store(i, j, *adam(own, i, j))
                return carry

            lax.fori_loop(0, tiles // step_tiles, body, 0)
        follow(3, SCHEDULE[3], [])
        swap.wait_send()

    for started in exchanges:
        started.wait_send()


def write_kernel(whole, new_master, new_first, new_second, codes_out, scales_out, master_out, first_out, second_out, sem):
    rows, cols = codes_out.shape
    count = 8
    step = rows // count
    copies = []

    def go(src, dst):
        copy = pltpu.make_async_copy(src, dst, sem.at[len(copies)])
        copy.start()
        copies.append(copy)

    for k in range(count):
        go(whole.at[pl.ds(k * step, step), pl.ds(0, cols)], codes_out.at[pl.ds(k * step, step), :])
    go(whole.at[:, pl.ds(cols, scales_out.shape[1])], scales_out)
    go(new_master, master_out)
    go(new_first, first_out)
    go(new_second, second_out)
    for copy in copies:
        copy.wait()


def per_device(master, gradient, first_moment, second_moment, max_norm, step_count):
    rows, width = master.shape
    cols = 2 * width
    scales = cols // BLOCK
    kept = 32 * rows
    full = cols + scales
    smem = pl.BlockSpec(memory_space=pltpu.SMEM)
    any_spec = pl.BlockSpec(memory_space=pl.ANY)
    vmem = pl.BlockSpec(memory_space=pltpu.VMEM)
    held = pl.pallas_call(
        gather_kernel,
        out_shape=tuple(pltpu.VMEM((rows, width), F32) for _ in range(3)) + (pltpu.VMEM((kept, full), BF16),),
        in_specs=[smem, smem] + [any_spec] * 4,
        out_specs=tuple(vmem for _ in range(4)),
        scratch_shapes=[
            pltpu.VMEM((4, rows, width), F32),
            pltpu.VMEM((4, rows, width), F32),
            pltpu.VMEM((PART, cols), F32),
            pltpu.VMEM((2, 4, PART, LANES), F32),
            pltpu.VMEM((2, 1, LANES), F32),
            pltpu.VMEM((22, 1, LANES), F32),
            pltpu.SemaphoreType.DMA((4,)),
            pltpu.SemaphoreType.DMA((2,)),
            pltpu.SemaphoreType.DMA((2,)),
            pltpu.SemaphoreType.DMA((2,)),
            pltpu.SemaphoreType.DMA((18,)),
            pltpu.SemaphoreType.DMA((LEAVES + 2,)),
        ],
        compiler_params=pltpu.CompilerParams(collective_id=0, has_side_effects=True, vmem_limit_bytes=16 * 2**20),
        name="update_and_gather",
    )(
        max_norm,
        step_count,
        *(
            pltpu.with_memory_space_constraint(a, pltpu.HBM)
            for a in (master, gradient, first_moment, second_moment)
        ),
    )
    new_master, new_first, new_second, whole = (
        pltpu.with_memory_space_constraint(a, pltpu.VMEM) for a in held
    )
    codes, block_scales, new_master, new_first, new_second = pl.pallas_call(
        write_kernel,
        out_shape=(
            jax.ShapeDtypeStruct((kept, cols), BF16),
            jax.ShapeDtypeStruct((kept, scales), BF16),
        )
        + tuple(jax.ShapeDtypeStruct((rows, width), F32) for _ in range(3)),
        in_specs=[vmem] * 4,
        out_specs=tuple(any_spec for _ in range(5)),
        scratch_shapes=[pltpu.SemaphoreType.DMA((12,))],
        compiler_params=pltpu.CompilerParams(vmem_limit_bytes=16 * 2**20),
        name="write_results",
    )(whole, new_master, new_first, new_second)
    return (new_master, new_first, new_second, codes, block_scales)


def solution(mesh):
    return jax.shard_map(
        per_device,
        mesh=mesh,
        in_specs=(P("shard", "pair"),) * 4 + (P(), P()),
        out_specs=(P("shard", "pair"),) * 3 + (P("pair", None),) * 2,
        check_vma=False,
    )
```
